32 devices in a mesh: task: 4 (over y, core), param: 8 (over z, x).
Axes of the slice: x: 2, y: 2, z: 4, core: 2. Of those that a mesh axis runs over, the one named last changes fastest.
Arguments:
- params: bfloat16 [16, 512, 4096], P('task', 'param'), may hold values from -6 to 6
- fisher: float32 [16, 512, 4096], P('task', 'param'), may hold values from 3e-06 to 1, as said below
Outputs:
- merged: bfloat16 [512, 4096], P('param')
The draws below stay inside these ranges and needn't reach their ends.
Inputs may be any that keep to these rules, and one draw needn't show every extreme that they name: `fisher`: every entry is positive; scales differ strongly between tasks and between regions of rows.
All inputs are finite; a program needn't handle non-finite values.
Results may differ from the reference program's by a relative error of at most 0.00045.
Values may be sent and summed in bfloat16 or wider, within the bound.
No kernel may reach another device: no remote copies, remote signals or barrier semaphores. Data moves between devices by JAX's collectives and lax.ppermute only.
A program may use at most 64 MiB of HBM per device.

```python
import math
import jax
import jax.numpy as jnp
from jax import lax

FF = 4096
TASKS = 16
ROWS = 512


def draw_fisher(key, part):
    first, second, third = jax.random.split(key, 3)
    region = jnp.exp(jax.random.uniform(first, (TASKS, 8), jnp.float32, math.log(1.0 / 256.0), 0.0))
    region = jnp.repeat(region, ROWS // 8, axis=1)
    base = jnp.exp(jax.random.uniform(second, (TASKS, ROWS, FF), jnp.float32, math.log(0.001), 0.0))
    return (base * region[:, :, None]).astype(jnp.float32)


def block_levels(own_key, dims, cuts, least, top_value):
    gain, own = 1.0, jax.random.fold_in(own_key, 6)
    for position, blocks in cuts:
        draws = jnp.exp(jax.random.uniform(jax.random.fold_in(own, position), (blocks,), jnp.float32, least / len(cuts), top_value / len(cuts)))
        gain = gain * jnp.repeat(draws, dims[position] // blocks).reshape([-1 if axis == position else 1 for axis in range(len(dims))])
    return gain


def scatter_about(own_key, dims, spread, bound, shards=(), kind=jnp.bfloat16):
    factor_of = block_levels(own_key, dims, shards, -0.22, 0.18) if shards else 1.0
    values = jax.random.normal(own_key, dims, jnp.float32) * spread * factor_of
    return jnp.minimum(jnp.maximum(values, -bound), bound).astype(kind)


def setup_inputs(seed: int = 0) -> dict:
    arg_keys = jax.random.split(jax.random.key(seed), 3)
    return {
        "params": scatter_about(arg_keys[0], (TASKS, ROWS, FF), 1.0, 6.0, ((0, 4), (1, 8))),
        "fisher": draw_fisher(jax.random.fold_in(arg_keys[2], 71), 0),
    }


def reference(params, fisher):
    peak = jnp.max(fisher, axis=(1, 2))
    total = jnp.sum(fisher, axis=(1, 2))
    count = float(ROWS * FF)
    factor = count * peak / total

    def one_task(carry, items):
        theta, info, top, mult = items
        weight = jnp.clip(info / top, 0.002, 0.25) * mult
        return (carry[0] + weight * theta.astype(jnp.float32), carry[1] + weight), None

    start = (jnp.zeros((ROWS, FF), jnp.float32), jnp.zeros((ROWS, FF), jnp.float32))
    sums, unused = lax.scan(one_task, start, (params, fisher, peak, factor))
    return (sums[0] / sums[1]).astype(jnp.bfloat16)
```

```python
import jax
import jax.numpy as jnp
from jax import lax
from jax.sharding import PartitionSpec as P


def swap(value, axis, bit):
    size = lax.axis_size(axis)
    return lax.ppermute(value, axis, [(i, i ^ bit) for i in range(size)])


def bits_of(axis):
    size = lax.axis_size(axis)
    return [1 << k for k in range(size.bit_length() - 1)]


def param_stats(fisher):
    peak = jnp.max(fisher, axis=(1, 2))
    total = jnp.sum(fisher, axis=(1, 2))
    for bit in bits_of("param"):
        stats = jnp.stack([peak, total])
        other = swap(stats, "param", bit)
        peak = jnp.maximum(peak, other[0])
        total = total + other[1]
    return peak, total


def keep_send(value, axis, bit):
    half = value.shape[1] // 2
    upper = (lax.axis_index(axis) & bit) != 0
    low, high = value[:, :half], value[:, half:]
    return jnp.where(upper, high, low), jnp.where(upper, low, high)


def local(params, fisher):
    peak, total = param_stats(fisher)
    count = float(fisher.shape[1] * lax.axis_size("param") * fisher.shape[2])
    factor = count * peak / total
    weight = jnp.clip(fisher / peak[:, None, None], 0.002, 0.25) * factor[:, None, None]
    numer = jnp.sum(weight * params.astype(jnp.float32), axis=0)
    denom = jnp.sum(weight, axis=0)
    part = jnp.stack([numer, denom])
    bits = bits_of("task")
    for bit in bits:
        keep, send = keep_send(part, "task", bit)
        part = keep + swap(send, "task", bit)
    merged = (part[0] / part[1]).astype(jnp.bfloat16)
    for bit in reversed(bits):
        other = swap(merged, "task", bit)
        upper = (lax.axis_index("task") & bit) != 0
        merged = jnp.where(upper, jnp.concatenate([other, merged]), jnp.concatenate([merged, other]))
    return merged


def solution(mesh):
    in_specs = (P("task", "param", None), P("task", "param", None))
    out_specs = P("param", None)
    return jax.shard_map(local, mesh=mesh, in_specs=in_specs, out_specs=out_specs, check_vma=False)
```

```python
import functools

import jax
import jax.numpy as jnp
from jax import lax
from jax.experimental import pallas as pl
from jax.experimental.pallas import tpu as pltpu
from jax.sharding import PartitionSpec as P

CHUNKS = 2
STEP = 512
PIECES = 2
COST = 100
PARAMS = pltpu.CompilerParams(vmem_limit_bytes=16 * 1024 * 1024)
VMEM = pl.BlockSpec(memory_space=pltpu.VMEM)
SMEM = pl.BlockSpec(memory_space=pltpu.SMEM)
HBM = pl.BlockSpec(memory_space=pltpu.HBM)


def swap(value, axis, bit):
    size = lax.axis_size(axis)
    return lax.ppermute(value, axis, [(i, i ^ bit) for i in range(size)])


def bits_of(axis):
    size = lax.axis_size(axis)
    return [1 << k for k in range(size.bit_length() - 1)]


def side(axis, bit):
    return ((lax.axis_index(axis) & bit) != 0).astype(jnp.int32).reshape(1)


def stats_kernel(fisher_ref, stats_ref, fisher_out, sems):
    tasks, rows, width = fisher_out.shape
    step = rows // PIECES
    loads = []
    for task in range(tasks):
        for piece in range(PIECES):
            at = (task, pl.ds(piece * step, step))
            loads.append(pltpu.make_async_copy(fisher_ref.at[at], fisher_out.at[at], sems.at[len(loads)]))
    for load in loads:
        load.start()
    for task in range(tasks):
        top = added = None
        for piece in range(PIECES):
            loads[task * PIECES + piece].wait()
            for row in range(piece * step, piece * step + step, 8):
                for col in range(0, width, 1024):
                    block = fisher_out[task, row : row + 8, col : col + 1024]
                    top = block if top is None else jnp.maximum(top, block)
                    added = block if added is None else added + block
        stats_ref[task : task + 1] = jnp.full((1, 128), jnp.max(top), jnp.float32)
        stats_ref[tasks + task : tasks + task + 1] = jnp.full((1, 128), jnp.sum(added), jnp.float32)


def local_stats(fisher):
    tasks = fisher.shape[0]
    return pl.pallas_call(
        stats_kernel,
        in_specs=[HBM],
        out_specs=VMEM,
        out_shape=pltpu.VMEM((2 * tasks, 128), jnp.float32),
        scratch_shapes=[pltpu.VMEM(fisher.shape, jnp.float32), pltpu.SemaphoreType.DMA((tasks * PIECES,))],
        name="local_stats",
    )(fisher)


def joined(one_ref, two_ref):
    tasks = one_ref.shape[0] // 2
    one, two = one_ref[...], two_ref[...]
    return jnp.maximum(one[:tasks], two[:tasks]), one[tasks:] + two[tasks:]


def join_kernel(one_ref, two_ref, out_ref):
    tasks = one_ref.shape[0] // 2
    out_ref[:tasks], out_ref[tasks:] = joined(one_ref, two_ref)


def join(one, two):
    return pl.pallas_call(
        join_kernel, in_specs=[VMEM] * 2, out_specs=VMEM, out_shape=pltpu.VMEM(one.shape, one.dtype), compiler_params=PARAMS, name="join"
    )(one, two)


def coef_kernel(one_ref, two_ref, out_ref, *, count):
    peak, total = joined(one_ref, two_ref)
    scale = count / total
    factor = scale * peak
    for k, value in enumerate([scale, 0.002 * factor, 0.25 * factor]):
        for task in range(value.shape[0]):
            out_ref[k * value.shape[0] + task, 0] = value[task, 0]


def coefs(one, two, count):
    kind = pltpu.SMEM((3 * one.shape[0] // 2, 1), jnp.float32)
    return pl.pallas_call(
        functools.partial(coef_kernel, count=count),
        in_specs=[VMEM] * 2,
        out_specs=SMEM,
        out_shape=kind,
        compiler_params=PARAMS,
        name="coefs",
    )(one, two)


def weigh_kernel(half_ref, stats_ref, fisher_hbm, params_hbm, after_ref, out_ref, fisher_ref, params_ref, sems, *, col):
    tasks, rows, cols = fisher_ref.shape
    step = min(cols, STEP)
    start = pl.ds(pl.multiple_of(half_ref[0] * rows, rows), rows)
    loads = []
    for piece in range(cols // step):
        source, target = pl.ds(col + piece * step, step), pl.ds(piece * step, step)
        pair = [
            pltpu.make_async_copy(hbm.at[:, start, source], ref.at[:, :, target], sems.at[k, piece])
            for k, (hbm, ref) in enumerate([(fisher_hbm, fisher_ref), (params_hbm, params_ref)])
        ]
        for copy in pair:
            copy.start()
        loads.append(pair)
    coef = [tuple(stats_ref[k * tasks + task, 0] for k in range(3)) for task in range(tasks)]
    for piece in range(cols // step):
        for copy in loads[piece]:
            copy.wait()
        for row in range(0, rows, 8):
            place = (slice(row, row + 8), slice(piece * step, piece * step + step))
            numer = denom = None
            for task in range(tasks):
                by, least, most = coef[task]
                weight = jnp.minimum(jnp.maximum(fisher_ref[(task,) + place] * by, least), most)
                term = weight * params_ref[(task,) + place].astype(jnp.float32)
                numer = term if task == 0 else numer + term
                denom = weight if task == 0 else denom + weight
            out_ref[(0,) + place] = numer
            out_ref[(1,) + place] = denom


def weighted(params, fisher, one, block, rows, col, cols, after, name):
    tasks = fisher.shape[0]
    return pl.pallas_call(
        functools.partial(weigh_kernel, col=col),
        in_specs=[SMEM, SMEM, HBM, HBM, SMEM],
        out_specs=VMEM,
        out_shape=pltpu.VMEM((2, rows, cols), jnp.float32),
        scratch_shapes=[
            pltpu.VMEM((tasks, rows, cols), jnp.float32),
            pltpu.VMEM((tasks, rows, cols), jnp.bfloat16),
            pltpu.SemaphoreType.DMA((2, cols // min(cols, STEP))),
        ],
        cost_estimate=pl.CostEstimate(flops=8 * tasks * rows * cols * COST, transcendentals=0, bytes_accessed=6 * tasks * rows * cols),
        name=name,
    )(block, one, fisher, params, after)


def split_kernel(upper_ref, one_ref, two_ref, send_ref, keep_ref, token_ref):
    token_ref[0] = upper_ref[0]
    size = send_ref.shape[1]
    mine = pl.multiple_of(upper_ref[0] * size, size)
    theirs = pl.multiple_of((1 - upper_ref[0]) * size, size)
    for k in range(2):
        send_ref[k] = one_ref[k, pl.ds(theirs, size)] + two_ref[k, pl.ds(theirs, size)]
        keep_ref[k] = one_ref[k, pl.ds(mine, size)] + two_ref[k, pl.ds(mine, size)]


def split(upper, one, two):
    kind = pltpu.VMEM((2, one.shape[1] // 2, one.shape[2]), one.dtype)
    return pl.pallas_call(
        split_kernel, in_specs=[SMEM, VMEM, VMEM], out_specs=[VMEM, VMEM, SMEM], out_shape=[kind, kind, pltpu.SMEM((1,), jnp.int32)], compiler_params=PARAMS, name="split"
    )(upper, one, two)


def merge_kernel(one_ref, two_ref, out_ref):
    out_ref[...] = ((one_ref[0] + two_ref[0]) / (one_ref[1] + two_ref[1])).astype(out_ref.dtype)


def merge(one, two):
    kind = pltpu.VMEM(one.shape[1:], jnp.bfloat16)
    return pl.pallas_call(
        merge_kernel, in_specs=[VMEM] * 2, out_specs=VMEM, out_shape=kind, compiler_params=PARAMS, name="merge"
    )(one, two)


def stacked(upper, mine, other):
    return jnp.where(upper[0] != 0, jnp.concatenate([other, mine]), jnp.concatenate([mine, other]))


def local(params, fisher):
    tasks, rows, width = fisher.shape
    count = float(rows * lax.axis_size("param") * width)
    one = local_stats(fisher)
    *early, final = bits_of("param")
    for bit in early:
        one = join(one, swap(one, "param", bit))
    two = swap(one, "param", final)
    first, *rest = bits_of("task")
    half, cols = rows // 2, width // CHUNKS
    core = side("task", first)
    uppers = {bit: side("task", bit) for bit in rest}
    after, merged = core, []
    coef = coefs(one, two, count)
    for chunk in range(CHUNKS):
        send = weighted(params, fisher, coef, 1 - core, half, chunk * cols, cols, after, "weigh_send")
        keep = weighted(params, fisher, coef, core, half, chunk * cols, cols, after, "weigh_keep")
        other = swap(send, "task", first)
        for bit in rest:
            send, keep, after = split(uppers[bit], keep, other)
            other = swap(send, "task", bit)
        out = merge(keep, other)
        for bit in reversed(rest):
            out = stacked(uppers[bit], out, swap(out, "task", bit))
        merged.append(out)
    out = jnp.concatenate(merged, axis=1)
    return stacked(core, out, swap(out, "task", first))


def solution(mesh):
    in_specs = (P("task", "param", None), P("task", "param", None))
    out_specs = P("param", None)
    return jax.shard_map(local, mesh=mesh, in_specs=in_specs, out_specs=out_specs, check_vma=False)
```

```python
import functools

import jax
import jax.numpy as jnp
from jax import lax
from jax.experimental import pallas as pl
from jax.experimental.pallas import tpu as pltpu
from jax.sharding import PartitionSpec as P

MIDDLE = 125.0**0.5
SHIFT = 125.0**0.25
STEP = 512
PIECES = 2
COST = 10000
PARAMS = pltpu.CompilerParams(vmem_limit_bytes=16 * 1024 * 1024)
VMEM = pl.BlockSpec(memory_space=pltpu.VMEM)
SMEM = pl.BlockSpec(memory_space=pltpu.SMEM)
HBM = pl.BlockSpec(memory_space=pltpu.HBM)


def swap(value, axis, bit):
    size = lax.axis_size(axis)
    return lax.ppermute(value, axis, [(i, i ^ bit) for i in range(size)])


def bits_of(axis):
    size = lax.axis_size(axis)
    return [1 << k for k in range(size.bit_length() - 1)]


def side(axis, bit):
    return ((lax.axis_index(axis) & bit) != 0).astype(jnp.int32).reshape(1)


def stats_kernel(fisher_ref, stats_ref, fisher_out, sems):
    tasks, rows, width = fisher_out.shape
    step = rows // PIECES
    loads = []
    for task in range(tasks):
        for piece in range(PIECES):
            at = (task, pl.ds(piece * step, step))
            loads.append(pltpu.make_async_copy(fisher_ref.at[at], fisher_out.at[at], sems.at[len(loads)]))
    for load in loads:
        load.start()
    for task in range(tasks):
        top = added = None
        for piece in range(PIECES):
            loads[task * PIECES + piece].wait()
            for row in range(piece * step, piece * step + step, 8):
                for col in range(0, width, 1024):
                    block = fisher_out[task, row : row + 8, col : col + 1024]
                    top = block if top is None else jnp.maximum(top, block)
                    added = block if added is None else added + block
        stats_ref[task : task + 1] = jnp.full((1, 128), jnp.max(top), jnp.float32)
        stats_ref[tasks + task : tasks + task + 1] = jnp.full((1, 128), jnp.sum(added), jnp.float32)


def local_stats(fisher):
    tasks = fisher.shape[0]
    return pl.pallas_call(
        stats_kernel,
        in_specs=[HBM],
        out_specs=VMEM,
        out_shape=pltpu.VMEM((2 * tasks, 128), jnp.float32),
        scratch_shapes=[pltpu.VMEM(fisher.shape, jnp.float32), pltpu.SemaphoreType.DMA((tasks * PIECES,))],
        name="local_stats",
    )(fisher)


def joined(one_ref, two_ref):
    tasks = one_ref.shape[0] // 2
    one, two = one_ref[...], two_ref[...]
    return jnp.maximum(one[:tasks], two[:tasks]), one[tasks:] + two[tasks:]


def join_kernel(one_ref, two_ref, out_ref):
    tasks = one_ref.shape[0] // 2
    out_ref[:tasks], out_ref[tasks:] = joined(one_ref, two_ref)


def join(one, two):
    return pl.pallas_call(
        join_kernel, in_specs=[VMEM] * 2, out_specs=VMEM, out_shape=pltpu.VMEM(one.shape, one.dtype), compiler_params=PARAMS, name="join"
    )(one, two)


def coef_kernel(one_ref, two_ref, out_ref, *, count):
    peak, total = joined(one_ref, two_ref)
    scale = count / total
    factor = scale * peak
    for k, value in enumerate([scale, 0.002 * factor, 0.25 * factor]):
        for task in range(value.shape[0]):
            out_ref[k * value.shape[0] + task, 0] = value[task, 0]


def coefs(one, two, count):
    kind = pltpu.SMEM((3 * one.shape[0] // 2, 1), jnp.float32)
    return pl.pallas_call(
        functools.partial(coef_kernel, count=count),
        in_specs=[VMEM] * 2,
        out_specs=SMEM,
        out_shape=kind,
        compiler_params=PARAMS,
        name="coefs",
    )(one, two)


def weigh_kernel(half_ref, stats_ref, fisher_hbm, params_hbm, after_ref, out_ref, fisher_ref, params_ref, sems, *, col):
    tasks, rows, cols = fisher_ref.shape
    step = min(cols, STEP)
    start = pl.ds(pl.multiple_of(half_ref[0] * rows, rows), rows)
    loads = []
    for piece in range(cols // step):
        source, target = pl.ds(col + piece * step, step), pl.ds(piece * step, step)
        pair = [
            pltpu.make_async_copy(hbm.at[:, start, source], ref.at[:, :, target], sems.at[k, piece])
            for k, (hbm, ref) in enumerate([(fisher_hbm, fisher_ref), (params_hbm, params_ref)])
        ]
        for copy in pair:
            copy.start()
        loads.append(pair)
    coef = [tuple(stats_ref[k * tasks + task, 0] for k in range(3)) for task in range(tasks)]
    for piece in range(cols // step):
        for copy in loads[piece]:
            copy.wait()
        for row in range(0, rows, 8):
            place = (slice(row, row + 8), slice(piece * step, piece * step + step))
            numer = denom = None
            for task in range(tasks):
                by, least, most = coef[task]
                weight = jnp.minimum(jnp.maximum(fisher_ref[(task,) + place] * by, least), most)
                term = weight * params_ref[(task,) + place].astype(jnp.float32)
                numer = term if task == 0 else numer + term
                denom = weight if task == 0 else denom + weight
            out_ref[(0,) + place] = numer
            out_ref[(1,) + place] = denom


def weighted(params, fisher, one, block, rows, col, cols, after, name):
    tasks = fisher.shape[0]
    return pl.pallas_call(
        functools.partial(weigh_kernel, col=col),
        in_specs=[SMEM, SMEM, HBM, HBM, SMEM],
        out_specs=VMEM,
        out_shape=pltpu.VMEM((2, rows, cols), jnp.float32),
        scratch_shapes=[
            pltpu.VMEM((tasks, rows, cols), jnp.float32),
            pltpu.VMEM((tasks, rows, cols), jnp.bfloat16),
            pltpu.SemaphoreType.DMA((2, cols // min(cols, STEP))),
        ],
        cost_estimate=pl.CostEstimate(flops=8 * tasks * rows * cols * COST, transcendentals=0, bytes_accessed=6 * tasks * rows * cols),
        name=name,
    )(block, one, fisher, params, after)


def power64(value):
    for _ in range(6):
        value = value * value
    return value


def encode(numer, denom, out_ref):
    cols = numer.shape[1]
    high = numer.astype(jnp.bfloat16)
    out_ref[:, :cols] = high
    out_ref[:, cols : 2 * cols] = (numer - high.astype(jnp.float32)).astype(jnp.bfloat16)
    top = jnp.full((numer.shape[0], 128), jnp.max(denom), jnp.float32).astype(jnp.bfloat16)
    out_ref[:, 3 * cols :] = top
    ratio = denom * (MIDDLE / top[:, :1].astype(jnp.float32))
    above = ratio >= 1.0
    code = power64(ratio * jnp.where(above, 1.0 / SHIFT, SHIFT))
    out_ref[:, 2 * cols : 3 * cols] = jnp.where(above, code, -code).astype(jnp.bfloat16)


def decode(ref, rows):
    cols = (ref.shape[1] - 128) // 3
    numer = ref[rows, :cols].astype(jnp.float32) + ref[rows, cols : 2 * cols].astype(jnp.float32)
    code = ref[rows, 2 * cols : 3 * cols].astype(jnp.float32)
    ratio = jnp.exp2(jnp.log2(jnp.abs(code)) * (1.0 / 64.0)) * jnp.where(code > 0.0, SHIFT, 1.0 / SHIFT)
    top = ref[rows, 3 * cols : 3 * cols + 1].astype(jnp.float32)
    return numer, ratio * (top * (1.0 / MIDDLE))


def both(one_ref, two_ref, rows):
    if len(two_ref.shape) == 3:
        numer, denom = two_ref[0, rows], two_ref[1, rows]
    else:
        numer, denom = decode(two_ref, rows)
    return one_ref[0, rows] + numer, one_ref[1, rows] + denom


def split_kernel(upper_ref, one_ref, two_ref, send_ref, keep_ref, token_ref):
    token_ref[0] = upper_ref[0]
    size = keep_ref.shape[1]
    mine = pl.multiple_of(upper_ref[0] * size, size)
    theirs = pl.multiple_of((1 - upper_ref[0]) * size, size)
    encode(*both(one_ref, two_ref, pl.ds(theirs, size)), send_ref)
    keep_ref[0], keep_ref[1] = both(one_ref, two_ref, pl.ds(mine, size))


def split(upper, one, two):
    size, cols = one.shape[1] // 2, one.shape[2]
    kinds = [pltpu.VMEM((size, 3 * cols + 128), jnp.bfloat16), pltpu.VMEM((2, size, cols), one.dtype), pltpu.SMEM((1,), jnp.int32)]
    return pl.pallas_call(
        split_kernel, in_specs=[SMEM, VMEM, VMEM], out_specs=[VMEM, VMEM, SMEM], out_shape=kinds, compiler_params=PARAMS, name="split"
    )(upper, one, two)


def merge_kernel(one_ref, two_ref, out_ref):
    numer, denom = both(one_ref, two_ref, slice(None))
    out_ref[...] = (numer / denom).astype(out_ref.dtype)


def merge(one, two):
    kind = pltpu.VMEM(one.shape[1:], jnp.bfloat16)
    return pl.pallas_call(
        merge_kernel, in_specs=[VMEM] * 2, out_specs=VMEM, out_shape=kind, compiler_params=PARAMS, name="merge"
    )(one, two)


def stacked(upper, mine, other):
    return jnp.where(upper[0] != 0, jnp.concatenate([other, mine]), jnp.concatenate([mine, other]))


def local(params, fisher):
    tasks, rows, width = fisher.shape
    count = float(rows * lax.axis_size("param") * width)
    one = local_stats(fisher)
    *early, final = bits_of("param")
    for bit in early:
        one = join(one, swap(one, "param", bit))
    two = swap(one, "param", final)
    first, *rest = bits_of("task")
    half, lead = rows // 2, width * 5 // 8
    core = side("task", first)
    uppers = {bit: side("task", bit) for bit in rest}
    after, merged = core, []
    coef = coefs(one, two, count)
    for col, cols in ((0, lead), (lead, width - lead)):
        send = weighted(params, fisher, coef, 1 - core, half, col, cols, after, "weigh_send")
        keep = weighted(params, fisher, coef, core, half, col, cols, after, "weigh_keep")
        other = swap(send, "task", first)
        for bit in rest:
            send, keep, after = split(uppers[bit], keep, other)
            other = swap(send, "task", bit)
        out = merge(keep, other)
        for bit in reversed(rest):
            out = stacked(uppers[bit], out, swap(out, "task", bit))
        merged.append(stacked(core, out, swap(out, "task", first)))
    return jnp.concatenate(merged, axis=1)


def solution(mesh):
    in_specs = (P("task", "param", None), P("task", "param", None))
    out_specs = P("param", None)
    return jax.shard_map(local, mesh=mesh, in_specs=in_specs, out_specs=out_specs, check_vma=False)
```

```python
import functools
import math

import jax
import jax.numpy as jnp
from jax import lax
from jax.experimental import pallas as pl
from jax.experimental.pallas import tpu as pltpu
from jax.sharding import PartitionSpec as P

MIDDLE = 125.0**0.5
SHIFT = 125.0**0.25
STEP = 512
PIECES = 2
COST = 10000
FETCH_COST = 10000
FETCHED_COST = 10000
PARAMS = pltpu.CompilerParams(vmem_limit_bytes=16 * 1024 * 1024)
VMEM = pl.BlockSpec(memory_space=pltpu.VMEM)
SMEM = pl.BlockSpec(memory_space=pltpu.SMEM)
HBM = pl.BlockSpec(memory_space=pltpu.HBM)


def swap(value, axis, bit):
    size = lax.axis_size(axis)
    return lax.ppermute(value, axis, [(i, i ^ bit) for i in range(size)])


def bits_of(axis):
    size = lax.axis_size(axis)
    return [1 << k for k in range(size.bit_length() - 1)]


def side(axis, bit):
    return ((lax.axis_index(axis) & bit) != 0).astype(jnp.int32).reshape(1)


def stats_kernel(fisher_ref, stats_ref, fisher_out, sems):
    tasks, rows, width = fisher_out.shape
    step = rows // PIECES
    loads = []
    for task in range(tasks):
        for piece in range(PIECES):
            at = (task, pl.ds(piece * step, step))
            loads.append(pltpu.make_async_copy(fisher_ref.at[at], fisher_out.at[at], sems.at[len(loads)]))
    for load in loads:
        load.start()
    for task in range(tasks):
        top = added = None
        for piece in range(PIECES):
            loads[task * PIECES + piece].wait()
            for row in range(piece * step, piece * step + step, 8):
                for col in range(0, width, 1024):
                    block = fisher_out[task, row : row + 8, col : col + 1024]
                    top = block if top is None else jnp.maximum(top, block)
                    added = block if added is None else added + block
        stats_ref[task : task + 1] = jnp.full((1, 128), jnp.max(top), jnp.float32)
        stats_ref[tasks + task : tasks + task + 1] = jnp.full((1, 128), jnp.sum(added), jnp.float32)


def local_stats(fisher):
    tasks = fisher.shape[0]
    return pl.pallas_call(
        stats_kernel,
        in_specs=[HBM],
        out_specs=VMEM,
        out_shape=pltpu.VMEM((2 * tasks, 128), jnp.float32),
        scratch_shapes=[pltpu.VMEM(fisher.shape, jnp.float32), pltpu.SemaphoreType.DMA((tasks * PIECES,))],
        name="local_stats",
    )(fisher)


def joined(one_ref, two_ref):
    tasks = one_ref.shape[0] // 2
    one, two = one_ref[...], two_ref[...]
    return jnp.maximum(one[:tasks], two[:tasks]), one[tasks:] + two[tasks:]


def join_kernel(one_ref, two_ref, out_ref, scalars_ref):
    tasks = one_ref.shape[0] // 2
    peak, total = joined(one_ref, two_ref)
    out_ref[:tasks], out_ref[tasks:] = peak, total
    for task in range(tasks):
        scalars_ref[task, 0] = peak[task, 0]
        scalars_ref[tasks + task, 0] = total[task, 0]


def join(one, two):
    return pl.pallas_call(
        join_kernel,
        in_specs=[VMEM] * 2,
        out_specs=[VMEM, SMEM],
        out_shape=[pltpu.VMEM(one.shape, one.dtype), pltpu.SMEM((one.shape[0], 1), one.dtype)],
        compiler_params=PARAMS,
        name="join",
    )(one, two)


def coef_kernel(scalars_ref, two_ref, out_ref, *, count):
    tasks = two_ref.shape[0] // 2
    for task in range(tasks):
        peak = jnp.maximum(two_ref[task : task + 1], scalars_ref[task, 0])
        total = two_ref[tasks + task : tasks + task + 1] + scalars_ref[tasks + task, 0]
        scale = count / total
        factor = scale * peak
        for k, value in enumerate([scale, 0.002 * factor, 0.25 * factor]):
            out_ref[k * tasks + task, 0] = value[0, 0]


def coefs(scalars, two, count):
    kind = pltpu.SMEM((3 * two.shape[0] // 2, 1), jnp.float32)
    return pl.pallas_call(
        functools.partial(coef_kernel, count=count),
        in_specs=[SMEM, VMEM],
        out_specs=SMEM,
        out_shape=kind,
        compiler_params=PARAMS,
        name="coefs",
    )(scalars, two)


def fetch_kernel(half_ref, after_ref, fisher_hbm, params_hbm, fisher_ref, params_ref, sems, *, col):
    tasks, rows, cols = fisher_ref.shape
    start = pl.ds(pl.multiple_of(half_ref[0] * rows, rows), rows)
    copies = [
        pltpu.make_async_copy(hbm.at[:, start, pl.ds(col, cols)], ref, sems.at[k])
        for k, (hbm, ref) in enumerate([(fisher_hbm, fisher_ref), (params_hbm, params_ref)])
    ]
    for copy in copies:
        copy.start()
    for copy in copies:
        copy.wait()


def fetch(params, fisher, after, block, rows, col, cols):
    shape = (fisher.shape[0], rows, cols)
    return pl.pallas_call(
        functools.partial(fetch_kernel, col=col),
        in_specs=[SMEM, SMEM, HBM, HBM],
        out_specs=[VMEM] * 2,
        out_shape=[pltpu.VMEM(shape, jnp.float32), pltpu.VMEM(shape, jnp.bfloat16)],
        scratch_shapes=[pltpu.SemaphoreType.DMA((2,))],
        cost_estimate=pl.CostEstimate(flops=8 * math.prod(shape) * FETCH_COST, transcendentals=0, bytes_accessed=6 * math.prod(shape)),
        name="fetch",
    )(block, after, fisher, params)


def weigh_fetched_kernel(stats_ref, fisher_ref, params_ref, out_ref):
    rows, cols = fisher_ref.shape[1:]
    coef = coef_of(stats_ref, fisher_ref.shape[0])
    for col in range(0, cols, STEP):
        weigh(coef, fisher_ref, params_ref, out_ref, col, min(STEP, cols - col))


def weighted_fetched(params, fisher, coef, name):
    tasks, rows, cols = fisher.shape
    return pl.pallas_call(
        weigh_fetched_kernel,
        in_specs=[SMEM, VMEM, VMEM],
        out_specs=VMEM,
        out_shape=pltpu.VMEM((2, rows, cols), jnp.float32),
        cost_estimate=pl.CostEstimate(flops=8 * tasks * rows * cols * FETCHED_COST, transcendentals=0, bytes_accessed=6 * tasks * rows * cols),
        compiler_params=PARAMS,
        name=name,
    )(coef, fisher, params)


def coef_of(stats_ref, tasks):
    return [tuple(stats_ref[k * tasks + task, 0] for k in range(3)) for task in range(tasks)]


def weigh(coef, fisher_ref, params_ref, out_ref, col, step):
    for row in range(0, out_ref.shape[1], 8):
        place = (slice(row, row + 8), slice(col, col + step))
        numer = denom = None
        for task, (by, least, most) in enumerate(coef):
            weight = jnp.minimum(jnp.maximum(fisher_ref[(task,) + place] * by, least), most)
            term = weight * params_ref[(task,) + place].astype(jnp.float32)
            numer = term if task == 0 else numer + term
            denom = weight if task == 0 else denom + weight
        out_ref[(0,) + place] = numer
        out_ref[(1,) + place] = denom


def weigh_kernel(half_ref, stats_ref, fisher_hbm, params_hbm, after_ref, out_ref, fisher_ref, params_ref, sems, *, col):
    tasks, rows, cols = fisher_ref.shape
    step = min(cols, STEP)
    start = pl.ds(pl.multiple_of(half_ref[0] * rows, rows), rows)
    loads = []
    for piece in range(cols // step):
        source, target = pl.ds(col + piece * step, step), pl.ds(piece * step, step)
        pair = [
            pltpu.make_async_copy(hbm.at[:, start, source], ref.at[:, :, target], sems.at[k, piece])
            for k, (hbm, ref) in enumerate([(fisher_hbm, fisher_ref), (params_hbm, params_ref)])
        ]
        for copy in pair:
            copy.start()
        loads.append(pair)
    coef = coef_of(stats_ref, tasks)
    for piece in range(cols // step):
        for copy in loads[piece]:
            copy.wait()
        weigh(coef, fisher_ref, params_ref, out_ref, piece * step, step)


def weighted(params, fisher, one, block, rows, col, cols, after, name):
    tasks = fisher.shape[0]
    return pl.pallas_call(
        functools.partial(weigh_kernel, col=col),
        in_specs=[SMEM, SMEM, HBM, HBM, SMEM],
        out_specs=VMEM,
        out_shape=pltpu.VMEM((2, rows, cols), jnp.float32),
        scratch_shapes=[
            pltpu.VMEM((tasks, rows, cols), jnp.float32),
            pltpu.VMEM((tasks, rows, cols), jnp.bfloat16),
            pltpu.SemaphoreType.DMA((2, cols // min(cols, STEP))),
        ],
        cost_estimate=pl.CostEstimate(flops=8 * tasks * rows * cols * COST, transcendentals=0, bytes_accessed=6 * tasks * rows * cols),
        name=name,
    )(block, one, fisher, params, after)


def power64(value):
    for _ in range(6):
        value = value * value
    return value


def encode(numer, denom, out_ref):
    cols = numer.shape[1]
    high = numer.astype(jnp.bfloat16)
    out_ref[:, :cols] = high
    out_ref[:, cols : 2 * cols] = (numer - high.astype(jnp.float32)).astype(jnp.bfloat16)
    top = jnp.full((numer.shape[0], 128), jnp.max(denom), jnp.float32).astype(jnp.bfloat16)
    out_ref[:, 3 * cols :] = top
    ratio = denom * (MIDDLE / top[:, :1].astype(jnp.float32))
    above = ratio >= 1.0
    code = power64(ratio * jnp.where(above, 1.0 / SHIFT, SHIFT))
    out_ref[:, 2 * cols : 3 * cols] = jnp.where(above, code, -code).astype(jnp.bfloat16)


def decode(ref, rows):
    cols = (ref.shape[1] - 128) // 3
    numer = ref[rows, :cols].astype(jnp.float32) + ref[rows, cols : 2 * cols].astype(jnp.float32)
    code = ref[rows, 2 * cols : 3 * cols].astype(jnp.float32)
    ratio = jnp.exp2(jnp.log2(jnp.abs(code)) * (1.0 / 64.0)) * jnp.where(code > 0.0, SHIFT, 1.0 / SHIFT)
    top = ref[rows, 3 * cols : 3 * cols + 1].astype(jnp.float32)
    return numer, ratio * (top * (1.0 / MIDDLE))


def both(one_ref, two_ref, rows):
    if len(two_ref.shape) == 3:
        numer, denom = two_ref[0, rows], two_ref[1, rows]
    else:
        numer, denom = decode(two_ref, rows)
    return one_ref[0, rows] + numer, one_ref[1, rows] + denom


def split_kernel(upper_ref, one_ref, two_ref, send_ref, keep_ref, token_ref):
    token_ref[0] = upper_ref[0]
    size = keep_ref.shape[1]
    mine = pl.multiple_of(upper_ref[0] * size, size)
    theirs = pl.multiple_of((1 - upper_ref[0]) * size, size)
    encode(*both(one_ref, two_ref, pl.ds(theirs, size)), send_ref)
    keep_ref[0], keep_ref[1] = both(one_ref, two_ref, pl.ds(mine, size))


def split(upper, one, two):
    size, cols = one.shape[1] // 2, one.shape[2]
    kinds = [pltpu.VMEM((size, 3 * cols + 128), jnp.bfloat16), pltpu.VMEM((2, size, cols), one.dtype), pltpu.SMEM((1,), jnp.int32)]
    return pl.pallas_call(
        split_kernel, in_specs=[SMEM, VMEM, VMEM], out_specs=[VMEM, VMEM, SMEM], out_shape=kinds, compiler_params=PARAMS, name="split"
    )(upper, one, two)


def merge_kernel(one_ref, two_ref, out_ref):
    numer, denom = both(one_ref, two_ref, slice(None))
    out_ref[...] = (numer / denom).astype(out_ref.dtype)


def merge(one, two):
    kind = pltpu.VMEM(one.shape[1:], jnp.bfloat16)
    return pl.pallas_call(
        merge_kernel, in_specs=[VMEM] * 2, out_specs=VMEM, out_shape=kind, compiler_params=PARAMS, name="merge"
    )(one, two)


def stacked(upper, mine, other):
    return jnp.where(upper[0] != 0, jnp.concatenate([other, mine]), jnp.concatenate([mine, other]))


def local(params, fisher):
    tasks, rows, width = fisher.shape
    count = float(rows * lax.axis_size("param") * width)
    one = local_stats(fisher)
    *early, final = bits_of("param")
    for bit in early:
        one, scalars = join(one, swap(one, "param", bit))
    first, *rest = bits_of("task")
    half, lead = rows // 2, width * 5 // 8
    core = side("task", first)
    uppers = {bit: side("task", bit) for bit in rest}
    two = swap(one, "param", final)
    fetched = fetch(params, fisher, scalars, 1 - core, half, 0, lead)
    coef = coefs(scalars, two, count)
    after, whole = core, []
    for col, cols in ((0, lead), (lead, width - lead)):
        if col == 0:
            send = weighted_fetched(fetched[1], fetched[0], coef, "weigh_fetched")
        else:
            send = weighted(params, fisher, coef, 1 - core, half, col, cols, after, "weigh_send")
        keep = weighted(params, fisher, coef, core, half, col, cols, after, "weigh_keep")
        other = swap(send, "task", first)
        for bit in rest:
            send, keep, after = split(uppers[bit], keep, other)
            other = swap(send, "task", bit)
        out = merge(keep, other)
        for bit in reversed(rest):
            out = stacked(uppers[bit], out, swap(out, "task", bit))
        part = stacked(core, out, swap(out, "task", first))
        whole.append(part)
    return jnp.concatenate(whole, axis=1)


def solution(mesh):
    in_specs = (P("task", "param", None), P("task", "param", None))
    out_specs = P("param", None)
    return jax.shard_map(local, mesh=mesh, in_specs=in_specs, out_specs=out_specs, check_vma=False)
```
